32 devices in a mesh: grp: 2 (over y), tm: 4 (over z), space: 4 (over x, core).
Axes of the slice: x: 2, y: 2, z: 4, core: 2. Of those that a mesh axis runs over, the one named last changes fastest.
Arguments:
- forcing: float32 [32, 32, 8, 128], P(('grp', 'tm'), 'space'), parts along dimension 0, may hold values from -6 to 6
- start_field: float32 [64, 8, 128], P(('grp', 'space')), parts along dimension 0, may hold values from -6 to 6
- velocity: float32 [3, 32, 8, 128], P(None, 'space'), may hold values from -0.5 to 0.5
- diffusivity: float32 [2], P('grp'), parts along dimension 0, may hold values from 0.3 to 1
Outputs:
- iterate: float32 [32, 32, 8, 128], P(('grp', 'tm'), 'space'), parts along dimension 0
The draws below stay inside these ranges and needn't reach their ends.
There are 2 independent parts, one for each index of `grp`. The reference program is written for one: setup_inputs(seed, part) draws one part's arguments, and reference() takes and returns one part's arrays. A program takes and returns all parts, laid end to end along the dimension named above; an argument that names none is the same for every part. Nothing has to cross between parts.
All inputs are finite; a program needn't handle non-finite values.
Results may differ from the reference program's by a relative error of at most 0.0001.
Values sent between devices are 32-bit elements; how exact they have to be, the bound alone decides.
A program may use at most 64 MiB of HBM per device.

```python
import math
import jax
import jax.numpy as jnp

NX = 8
NY = 128
SWEEPS = 4
CYCLES = 1
NT = 16
NZ = 32


def levels(key, dims, pieces, smallest, top_value):
    level = 1.0
    for position, blocks in pieces:
        draws = jax.random.uniform(jax.random.fold_in(jax.random.fold_in(key, 6), position), (blocks,), jnp.float32, smallest / len(pieces), top_value / len(pieces))
        level = level * jnp.repeat(jnp.exp(draws), dims[position] // blocks).reshape((-1,) + (1,) * (len(dims) - 1 - position))
    return level


def centred(own_key, extent, spread, limit, cuts=(), held_as=jnp.bfloat16):
    gain = levels(own_key, extent, cuts, -0.22, 0.18) if cuts else 1.0
    drawn = jax.random.normal(own_key, extent, jnp.float32) * spread * gain
    return jnp.minimum(jnp.maximum(drawn, -limit), limit).astype(held_as)


def setup_inputs(seed: int = 0, part: int = 0) -> dict:
    arg_keys = jax.random.split(jax.random.key(seed), 5)
    part_splits = jax.random.split(jax.random.fold_in(arg_keys[4], part), 5)
    return {
        "forcing": centred(part_splits[0], (NT, NZ, NX, NY), 1.0, 6.0, ((0, 4), (1, 4)), jnp.float32),
        "start_field": centred(part_splits[1], (NZ, NX, NY), 1.0, 6.0, ((0, 4),), jnp.float32),
        "velocity": jnp.clip(jax.random.uniform(arg_keys[2], (3, NZ, NX, NY), jnp.float32, -0.5, 0.5) * levels(arg_keys[2], (3, NZ, NX, NY), ((1, 4),), -0.4, 0.0), -0.5, 0.5),
        "diffusivity": jnp.clip(jnp.exp(jax.random.uniform(part_splits[3], (1,), jnp.float32, math.log(0.3), math.log(1.0))), 0.3, 1.0),
    }


time_unit = 0.5


def neighbour_sum(padded, velocity, kappa_value):
    middle = padded[..., 1:-1, :, :]
    higher = padded[..., 2:, :, :]
    beneath = padded[..., :-2, :, :]
    east_side = jnp.roll(middle, -1, axis=-2)
    west_side = jnp.roll(middle, 1, axis=-2)
    north_side = jnp.roll(middle, -1, axis=-1)
    south_side = jnp.roll(middle, 1, axis=-1)
    diffused = kappa_value * (higher + beneath + east_side + west_side + north_side + south_side)
    carried = velocity[0] * (higher - beneath) + velocity[1] * (east_side - west_side) + velocity[2] * (north_side - south_side)
    return diffused - 0.5 * carried


def propagate(source, velocity, kappa_value, time_step):
    diagonal = 1.0 + 6.0 * time_step * kappa_value
    widths = [(0, 0)] * (source.ndim - 3) + [(1, 1), (0, 0), (0, 0)]
    values = source
    for repeat in range(SWEEPS):
        padded = jnp.pad(values, widths)
        values = (source + time_step * neighbour_sum(padded, velocity, kappa_value)) / diagonal
    return values


def relax_points(iterate, forcing, start, velocity, kappa_value, time_step):
    blocks = iterate.shape[0] // 4
    carried = jnp.concatenate([start[None], iterate[3::4][:blocks - 1]], axis=0)
    first_point = propagate(carried, velocity, kappa_value, time_step) + forcing[0::4]
    second_point = propagate(first_point, velocity, kappa_value, time_step) + forcing[1::4]
    third_point = propagate(second_point, velocity, kappa_value, time_step) + forcing[2::4]
    stacked = jnp.stack([first_point, second_point, third_point, iterate[3::4]], axis=1)
    return stacked.reshape(iterate.shape)


def solve_level(level_index, iterate, forcing, start, velocity, kappa_value):
    time_step = time_unit * 4.0 ** level_index
    if iterate.shape[0] == 4:
        previous = start
        points = []
        for offset in range(4):
            previous = propagate(previous, velocity, kappa_value, time_step) + forcing[offset]
            points.append(previous)
        return jnp.stack(points)
    iterate = relax_points(iterate, forcing, start, velocity, kappa_value, time_step)
    if level_index == 0:
        coarse_points = propagate(iterate[2::4], velocity, kappa_value, time_step) + forcing[3::4]
        iterate = iterate.at[3::4].set(coarse_points)
        iterate = relax_points(iterate, forcing, start, velocity, kappa_value, time_step)
    residual = forcing[3::4] + propagate(iterate[2::4], velocity, kappa_value, time_step) - iterate[3::4]
    correction = solve_level(level_index + 1, jnp.zeros_like(residual), residual, jnp.zeros_like(start), velocity, kappa_value)
    iterate = iterate.at[3::4].add(correction)
    return relax_points(iterate, forcing, start, velocity, kappa_value, time_step)


def reference(forcing, start_field, velocity, diffusivity):
    kappa_value = diffusivity[0]
    iterate = jnp.zeros_like(forcing)
    for repeat in range(CYCLES):
        iterate = solve_level(0, iterate, forcing, start_field, velocity, kappa_value)
    return iterate
```

```python
import functools

import jax
import jax.numpy as jnp
from jax import lax
from jax.experimental import pallas as pl
from jax.experimental.pallas import tpu as pltpu
from jax.sharding import PartitionSpec as P

SWEEPS = 4
BLOCK = 4

time_unit = 0.5


def passed_along(value, axis, steps):
    count = lax.axis_size(axis)
    leading, last = (max(0, -steps), min(count, count - steps))
    return lax.ppermute(value, axis, [(source, source + steps) for source in range(leading, last)])


def neighbour_sum(padded, velocity, kappa_value):
    middle = padded[1:-1]
    higher = padded[2:]
    beneath = padded[:-2]
    east_side = jnp.roll(middle, -1, axis=1)
    west_side = jnp.roll(middle, 1, axis=1)
    north_side = jnp.roll(middle, -1, axis=2)
    south_side = jnp.roll(middle, 1, axis=2)
    diffused = kappa_value * (higher + beneath + east_side + west_side + north_side + south_side)
    carried = (
        velocity[0] * (higher - beneath)
        + velocity[1] * (east_side - west_side)
        + velocity[2] * (north_side - south_side)
    )
    return diffused - 0.5 * carried


def deep_local(forcing, start_field, velocity, diffusivity):
    kappa_value = diffusivity[0]
    time_count = lax.axis_size("tm")
    time_rank = lax.axis_index("tm")
    coarse_levels = (time_count.bit_length() - 1) // 2
    slab_rows = forcing.shape[1]
    forcing_used, start_used, velocity_all = (
        lax.all_gather(forcing, "space", axis=1, tiled=True),
        lax.all_gather(start_field, "space", axis=0, tiled=True),
        lax.all_gather(velocity, "space", axis=1, tiled=True),
    )

    def propagate(source, time_step):
        diagonal = 1.0 + 6.0 * time_step * kappa_value
        values = source
        for repeat in range(SWEEPS):
            padded = jnp.pad(values, ((1, 1), (0, 0), (0, 0)))
            values = (
                source + time_step * neighbour_sum(padded, velocity_all, kappa_value)
            ) / diagonal
        return values

    def advance(values, stride):
        return passed_along(values, "tm", stride)

    starting = (time_rank == 0).astype(jnp.float32)

    def relax_fine(iterate):
        previous = advance(iterate[3], 1) + starting * start_used
        first_point = propagate(previous, time_unit) + forcing_used[0]
        second_point = propagate(first_point, time_unit) + forcing_used[1]
        third_point = propagate(second_point, time_unit) + forcing_used[2]
        return jnp.stack([first_point, second_point, third_point, iterate[3]])

    def solve_coarse(level_index, right_side):
        stride = 4 ** (level_index - 1)
        time_step = time_unit * 4.0**level_index
        active = (time_rank + 1) % stride == 0
        position = (time_rank + 1) // stride

        def step_where(values, chosen):
            return jnp.where(
                chosen, propagate(advance(values, stride), time_step) + right_side, values
            )

        correction = jnp.zeros_like(right_side)
        if level_index == coarse_levels:
            for offset in range(1, 5):
                correction = step_where(correction, active & (position == offset))
            return jnp.where(active, correction, 0.0)

        def relax_points(values):
            for offset in range(1, 4):
                values = step_where(values, active & (position % 4 == offset))
            return values

        correction = relax_points(correction)
        residual = right_side + propagate(advance(correction, stride), time_step) - correction
        correction = correction + solve_coarse(level_index + 1, residual)
        correction = relax_points(correction)
        return jnp.where(active, correction, 0.0)

    iterate = jnp.zeros_like(forcing_used)
    iterate = relax_fine(iterate)
    coarse_point = propagate(iterate[2], time_unit) + forcing_used[3]
    iterate = jnp.concatenate([iterate[:3], coarse_point[None]], axis=0)
    iterate = relax_fine(iterate)
    residual = forcing_used[3] + propagate(iterate[2], time_unit) - iterate[3]
    correction = solve_coarse(1, residual)
    iterate = jnp.concatenate([iterate[:3], (iterate[3] + correction)[None]], axis=0)
    iterate = relax_fine(iterate)
    iterate = lax.dynamic_slice_in_dim(iterate, lax.axis_index("space") * slab_rows, slab_rows, 1)
    return iterate


def kernel(
    spaces, times,
    f_ref, u_ref, v_ref, k_ref, out_ref,
    fields, vel, tab, scaled, ping, pong, chain, got, echo, err,
    local_sem, near_send, near_recv, far_send, far_recv, pass_send, pass_recv,
    hop_send, hop_recv, swap_send, swap_recv,
):
    slab = f_ref.shape[1]
    depth = vel.shape[1]
    s = lax.axis_index("space")
    t = lax.axis_index("tm")
    mate = s + 1 - 2 * lax.rem(s, 2)
    base = pl.multiple_of(s * slab, slab)
    pairs = spaces // 2
    kappa = k_ref[0]

    own = pl.ds(base, slab)
    pieces = [vel.at[:, own]] + [fields.at[i, own] for i in range(BLOCK + 1)]
    sources = [v_ref, u_ref] + [f_ref.at[i] for i in range(BLOCK)]
    locals_ = [
        pltpu.make_async_copy(a, b, local_sem.at[i])
        for i, (a, b) in enumerate(zip(sources, pieces))
    ]
    for copy in locals_:
        copy.start()

    barrier = pltpu.get_barrier_semaphore()
    for k in range(1, spaces):
        pl.semaphore_signal(
            barrier, inc=1, device_id={"space": lax.rem(s + k, spaces)},
            device_id_type=pl.DeviceIdType.MESH)
    for k in range(1, times):
        pl.semaphore_signal(
            barrier, inc=1, device_id={"tm": lax.rem(t + k, times)},
            device_id_type=pl.DeviceIdType.MESH)
    pl.semaphore_wait(barrier, spaces - 1 + times - 1)

    def piece(i, owner):
        rows = pl.ds(pl.multiple_of(owner * slab, slab), slab)
        return vel.at[:, rows] if i == 0 else fields.at[i - 1, rows]

    def far_copy(i, k):
        return pltpu.make_async_remote_copy(
            piece(i, s), piece(i, s), far_send.at[k - 1, i], far_recv.at[k - 1, i],
            device_id={"space": lax.rem(s + 2 * k, spaces)},
            device_id_type=pl.DeviceIdType.MESH)

    def near_copy(i):
        return pltpu.make_async_remote_copy(
            piece(i, s), piece(i, s), near_send.at[i], near_recv.at[i],
            device_id={"space": mate}, device_id_type=pl.DeviceIdType.MESH)

    def origin(k):
        return lax.rem(s - 2 * k + spaces, spaces)

    def pass_copy(i, k):
        return pltpu.make_async_remote_copy(
            piece(i, origin(k)), piece(i, origin(k)), pass_send.at[k - 1, i], pass_recv.at[k - 1, i],
            device_id={"space": mate}, device_id_type=pl.DeviceIdType.MESH)

    def far_arrived(i, k):
        return pltpu.make_async_copy(piece(i, origin(k)), piece(i, origin(k)), far_recv.at[k - 1, i])

    total = BLOCK + 2
    order = [0, 1, 2, 3, 4, 5]
    for i in order:
        locals_[i].wait()
        for k in range(1, pairs):
            far_copy(i, k).start()
        near_copy(i).start()

    def collect(i):
        for k in range(1, pairs):
            far_copy(i, k).wait_recv()
            pass_copy(i, k).start()
        near_copy(i).wait_recv()
        for k in range(1, pairs):
            pass_copy(i, k).wait_recv()

    steps = (time_unit, time_unit * 4.0)
    inverse = []
    for h in steps:
        inverse.append(1.0 / jnp.full((8, 128), 1.0 + 6.0 * h * kappa, jnp.float32))

    def make_tables(level):
        h = steps[level]

        def plane(z, carry):
            for d in range(3):
                half = 0.5 * vel[d, z]
                tab[level, 2 * d, z] = (h * inverse[level]) * (kappa - half)
                tab[level, 2 * d + 1, z] = (h * inverse[level]) * (kappa + half)
            return carry

        lax.fori_loop(0, depth, plane, 0)

    def phi(level, load, store):
        put0 = lambda z, v: ping.__setitem__(z, v)
        stages = [
            (load, lambda z, v: ping.__setitem__(z, v)),
            (lambda z: ping[z], lambda z, v: pong.__setitem__(z, v)),
            (lambda z: pong[z], lambda z, v: ping.__setitem__(z, v)),
            (lambda z: ping[z], store),
        ]
        for number, (read, write) in enumerate(stages):
            below, here = None, read(0)
            for z in range(depth):
                above = read(z + 1) if z + 1 < depth else None
                if number == 0:
                    value = here * inverse[level]
                    scaled[z] = value
                else:
                    value = scaled[z]
                x = tab[level, 2, z] * pltpu.roll(here, 7, 0) + tab[level, 3, z] * pltpu.roll(here, 1, 0)
                y = tab[level, 4, z] * pltpu.roll(here, 127, 1) + tab[level, 5, z] * pltpu.roll(here, 1, 1)
                if above is not None:
                    value = value + tab[level, 0, z] * above
                if below is not None:
                    value = value + tab[level, 1, z] * below
                value = value + (x + y)
                write(z, value)
                below, here = here, above

    collect(0)
    make_tables(0)

    collect(1)
    collect(2)

    @pl.when(t == 0)
    def _():
        phi(0, lambda z: fields[0, z],
            lambda z, v: chain.__setitem__((0, z), v + fields[1, z]))

    @pl.when(t > 0)
    def _():
        chain[0] = fields[1]

    for i in range(1, BLOCK):
        collect(i + 2)
        if i < BLOCK:
            pass

    def advance(i, carry):
        phi(0, lambda z: chain[i - 1, z],
            lambda z, v: chain.__setitem__((i, z), v + fields[i + 1, z]))
        return carry

    lax.fori_loop(1, BLOCK, advance, 0)

    half = depth // 2
    rows = pl.ds(pl.multiple_of(lax.rem(s, 2) * half, half), half)

    def hop_copy(k):
        return pltpu.make_async_remote_copy(
            chain.at[BLOCK - 1, rows], got.at[t, rows], hop_send.at[k - 1], hop_recv.at[t],
            device_id={"tm": lax.rem(t + k, times)}, device_id_type=pl.DeviceIdType.MESH)

    for k in range(times - 1, 0, -1):
        @pl.when(t + k < times)
        def _():
            hop_copy(k).start()

    make_tables(1)

    def swap_copy(j):
        return pltpu.make_async_remote_copy(
            got.at[j, rows], got.at[j, rows], swap_send.at[j], swap_recv.at[j],
            device_id={"space": mate}, device_id_type=pl.DeviceIdType.MESH)

    def hop_arrival(j):
        return pltpu.make_async_remote_copy(
            chain.at[BLOCK - 1, rows], got.at[j, rows], hop_send.at[0], hop_recv.at[j],
            device_id={"tm": lax.rem(t + 1, times)}, device_id_type=pl.DeviceIdType.MESH)

    for j in range(times - 2, -1, -1):
        @pl.when(t > j)
        def _():
            hop_arrival(j).wait_recv()
            swap_copy(j).start()
            swap_copy(j).wait_recv()
            echo[j] = got[j]

            def again(i, carry):
                phi(0, lambda z: echo[j, z], lambda z, v: echo.__setitem__((j, z), v))
                return carry

            lax.fori_loop(0, BLOCK, again, 0)

    @pl.when(t == 0)
    def _():
        for i in range(BLOCK):
            out_ref[i] = chain[i, own]

    @pl.when(t > 0)
    def _():
        err[0] = jnp.zeros(err.shape[1:], jnp.float32)
        err[1] = echo[0]

        def correct(m, carry):
            phi(1, lambda z: err[m - 1, z],
                lambda z, v: err.__setitem__((m, z), v + echo[m - 1, z]))
            return carry

        lax.fori_loop(2, t + 1, correct, 0)
        echo[0] = got[t - 1] + err[t - 1]

        def relax(i, carry):
            phi(0, lambda z: echo[0, z], lambda z, v: echo.__setitem__((0, z), v))
            out_ref[i] = chain[i, own] + echo[0, own]
            return carry

        lax.fori_loop(0, BLOCK - 1, relax, 0)
        out_ref[BLOCK - 1] = chain[BLOCK - 1, own] + err[t, own]

    for i in range(total):
        near_copy(i).wait_send()
        for k in range(1, pairs):
            far_copy(i, k).wait_send()
            pass_copy(i, k).wait_send()
    for k in range(1, times):
        @pl.when(t + k < times)
        def _():
            hop_copy(k).wait_send()
    for j in range(times - 1):
        @pl.when(t > j)
        def _():
            swap_copy(j).wait_send()


def shallow_local(forcing, start_field, velocity, diffusivity):
    spaces, times = lax.axis_size("space"), lax.axis_size("tm")
    slab = forcing.shape[1]
    field = (spaces * slab,) + forcing.shape[2:]
    dma = pltpu.SemaphoreType.DMA
    vmem = lambda *shape: pltpu.VMEM(shape + field, jnp.float32)
    pieces, pairs = BLOCK + 2, max(spaces // 2 - 1, 1)
    return pl.pallas_call(
        functools.partial(kernel, spaces, times),
        out_shape=jax.ShapeDtypeStruct(forcing.shape, forcing.dtype),
        in_specs=[pl.BlockSpec(memory_space=pl.ANY)] * 3 + [pl.BlockSpec(memory_space=pltpu.SMEM)],
        out_specs=pl.BlockSpec(memory_space=pltpu.VMEM),
        scratch_shapes=[
            vmem(BLOCK + 1), vmem(3), vmem(2, 6), vmem(), vmem(), vmem(),
            vmem(BLOCK), vmem(times), vmem(times), vmem(times + 1),
            dma((pieces,)), dma((pieces,)), dma((pieces,)),
            dma((pairs, pieces)), dma((pairs, pieces)), dma((pairs, pieces)), dma((pairs, pieces)),
            dma((times,)), dma((times,)), dma((times,)), dma((times,)),
        ],
        compiler_params=pltpu.CompilerParams(collective_id=0, has_side_effects=True),
    )(forcing, start_field, velocity, diffusivity)


def solution(mesh):
    placed = (
        P(("grp", "tm"), "space", None, None),
        P(("grp", "space"), None, None),
        P(None, "space", None, None),
        P("grp"),
    )
    one_level = mesh.shape["tm"] == BLOCK and mesh.shape["space"] % 2 == 0
    return jax.shard_map(
        shallow_local if one_level else deep_local,
        mesh=mesh,
        in_specs=placed,
        out_specs=P(("grp", "tm"), "space", None, None),
        check_vma=False,
    )
```

```python
import functools

import jax
import jax.numpy as jnp
from jax import lax
from jax.experimental import pallas as pl
from jax.experimental.pallas import tpu as pltpu
from jax.sharding import PartitionSpec as P

SWEEPS = 4
BLOCK = 4

time_unit = 0.5


def passed_along(value, axis, steps):
    count = lax.axis_size(axis)
    leading, last = (max(0, -steps), min(count, count - steps))
    return lax.ppermute(value, axis, [(source, source + steps) for source in range(leading, last)])


def neighbour_sum(padded, velocity, kappa_value):
    middle = padded[1:-1]
    higher = padded[2:]
    beneath = padded[:-2]
    east_side = jnp.roll(middle, -1, axis=1)
    west_side = jnp.roll(middle, 1, axis=1)
    north_side = jnp.roll(middle, -1, axis=2)
    south_side = jnp.roll(middle, 1, axis=2)
    diffused = kappa_value * (higher + beneath + east_side + west_side + north_side + south_side)
    carried = (
        velocity[0] * (higher - beneath)
        + velocity[1] * (east_side - west_side)
        + velocity[2] * (north_side - south_side)
    )
    return diffused - 0.5 * carried


def deep_local(forcing, start_field, velocity, diffusivity):
    kappa_value = diffusivity[0]
    time_count = lax.axis_size("tm")
    time_rank = lax.axis_index("tm")
    coarse_levels = (time_count.bit_length() - 1) // 2
    slab_rows = forcing.shape[1]
    forcing_used, start_used, velocity_all = (
        lax.all_gather(forcing, "space", axis=1, tiled=True),
        lax.all_gather(start_field, "space", axis=0, tiled=True),
        lax.all_gather(velocity, "space", axis=1, tiled=True),
    )

    def propagate(source, time_step):
        diagonal = 1.0 + 6.0 * time_step * kappa_value
        values = source
        for repeat in range(SWEEPS):
            padded = jnp.pad(values, ((1, 1), (0, 0), (0, 0)))
            values = (
                source + time_step * neighbour_sum(padded, velocity_all, kappa_value)
            ) / diagonal
        return values

    def advance(values, stride):
        return passed_along(values, "tm", stride)

    starting = (time_rank == 0).astype(jnp.float32)

    def relax_fine(iterate):
        previous = advance(iterate[3], 1) + starting * start_used
        first_point = propagate(previous, time_unit) + forcing_used[0]
        second_point = propagate(first_point, time_unit) + forcing_used[1]
        third_point = propagate(second_point, time_unit) + forcing_used[2]
        return jnp.stack([first_point, second_point, third_point, iterate[3]])

    def solve_coarse(level_index, right_side):
        stride = 4 ** (level_index - 1)
        time_step = time_unit * 4.0**level_index
        active = (time_rank + 1) % stride == 0
        position = (time_rank + 1) // stride

        def step_where(values, chosen):
            return jnp.where(
                chosen, propagate(advance(values, stride), time_step) + right_side, values
            )

        correction = jnp.zeros_like(right_side)
        if level_index == coarse_levels:
            for offset in range(1, 5):
                correction = step_where(correction, active & (position == offset))
            return jnp.where(active, correction, 0.0)

        def relax_points(values):
            for offset in range(1, 4):
                values = step_where(values, active & (position % 4 == offset))
            return values

        correction = relax_points(correction)
        residual = right_side + propagate(advance(correction, stride), time_step) - correction
        correction = correction + solve_coarse(level_index + 1, residual)
        correction = relax_points(correction)
        return jnp.where(active, correction, 0.0)

    iterate = jnp.zeros_like(forcing_used)
    iterate = relax_fine(iterate)
    coarse_point = propagate(iterate[2], time_unit) + forcing_used[3]
    iterate = jnp.concatenate([iterate[:3], coarse_point[None]], axis=0)
    iterate = relax_fine(iterate)
    residual = forcing_used[3] + propagate(iterate[2], time_unit) - iterate[3]
    correction = solve_coarse(1, residual)
    iterate = jnp.concatenate([iterate[:3], (iterate[3] + correction)[None]], axis=0)
    iterate = relax_fine(iterate)
    iterate = lax.dynamic_slice_in_dim(iterate, lax.axis_index("space") * slab_rows, slab_rows, 1)
    return iterate


def kernel(
    spaces, times,
    f_ref, u_ref, v_ref, k_ref, out_ref,
    slabs, tab, scaled, ping, pong, chain, got, echo, prev, err,
    local_sem, near_send, near_recv, far_send, far_recv, pass_send, pass_recv,
    hop_send, hop_recv, swap_send, swap_recv, ready,
):
    MESH = pl.DeviceIdType.MESH
    slab = f_ref.shape[1]
    depth = spaces * slab
    pad = (tab.shape[2] - depth) // 2
    s = lax.axis_index("space")
    t = lax.axis_index("tm")
    mate = s + 1 - 2 * lax.rem(s, 2)
    pairs = spaces // 2
    kappa = k_ref[0]
    own = pl.ds(pl.multiple_of(s * slab, slab), slab)
    start, force = 3, 4

    pieces = [(0, force), (force, force + 2), (force + 2, force + 3), (force + 3, force + 4)]
    locals_ = [
        pltpu.make_async_copy(v_ref, slabs.at[s, pl.ds(0, 3)], local_sem.at[0]),
        pltpu.make_async_copy(u_ref, slabs.at[s, start], local_sem.at[1]),
        pltpu.make_async_copy(f_ref, slabs.at[s, pl.ds(force, BLOCK)], local_sem.at[2]),
    ]
    for copy in locals_:
        copy.start()

    barrier = pltpu.get_barrier_semaphore()
    for k in range(1, spaces):
        pl.semaphore_signal(
            barrier, inc=1, device_id={"space": lax.rem(s + k, spaces)}, device_id_type=MESH)

    @pl.when(t > 0)
    def _():
        pl.semaphore_signal(barrier, inc=1, device_id={"tm": t - 1}, device_id_type=MESH)

    @pl.when(t < times - 1)
    def _():
        pl.semaphore_signal(barrier, inc=1, device_id={"tm": t + 1}, device_id_type=MESH)

    zero = jnp.zeros((8, 128), jnp.float32)
    for z in list(range(pad)) + list(range(pad + depth, depth + 2 * pad)):
        for level in range(2):
            for c in range(6):
                tab[level, c, z] = zero
        for i in range(BLOCK):
            chain[i, z] = zero
        prev[z] = zero
        err[0, z] = zero
        err[1, z] = zero

    def ends(low, high):
        return jnp.where(t > 0, low, 0) + jnp.where(t < times - 1, high, 0)

    pl.semaphore_wait(barrier, spaces - 1 + ends(1, 1))

    def piece(i, owner):
        low, high = pieces[i]
        return slabs.at[owner, pl.ds(low, high - low)]

    def origin(k, of=None):
        return lax.rem((s if of is None else of) - 2 * k + spaces, spaces)

    def remote(src, send, recv, **target):
        return pltpu.make_async_remote_copy(
            src, src, send, recv, device_id=target, device_id_type=MESH)

    def far_copy(i, k):
        return remote(piece(i, s), far_send.at[k - 1, i], far_recv.at[k - 1, i],
                      space=lax.rem(s + 2 * k, spaces))

    def near_copy(i):
        return remote(piece(i, s), near_send.at[i], near_recv.at[i], space=mate)

    def pass_copy(i, k):
        return remote(piece(i, origin(k)), pass_send.at[k - 1, i], pass_recv.at[k - 1, i],
                      space=mate)

    for i in range(len(pieces)):
        for copy in {0: locals_[:2], 1: locals_[2:]}.get(i, []):
            copy.wait()
        for k in range(1, pairs):
            far_copy(i, k).start()
        near_copy(i).start()

    steps = (time_unit, time_unit * 4.0)
    inverse = [1.0 / jnp.full((8, 128), 1.0 + 6.0 * h * kappa, jnp.float32) for h in steps]

    def make_tables(owner):
        scale = steps[0] * inverse[0]
        middle, side = scale * kappa, scale * 0.5
        first = pad + owner * slab
        for z in range(slab):
            for d in range(3):
                part = side * slabs[owner, d, z]
                tab[0, 2 * d, first + z] = middle - part
                tab[0, 2 * d + 1, first + z] = middle + part

    make_tables(s)
    near_copy(0).wait_recv()
    make_tables(mate)

    for k in range(2, times):
        @pl.when((t > 0) & (t - 1 + k < times))
        def _():
            pl.semaphore_signal(ready.at[k], inc=1, device_id={"tm": t - 1}, device_id_type=MESH)

        @pl.when(t + k < times)
        def _():
            pl.semaphore_wait(ready.at[k], 1)

    def forward(i):
        for k in range(1, pairs):
            far_copy(i, k).wait_recv()
            pass_copy(i, k).start()

    def settle(i):
        near_copy(i).wait_recv()
        for k in range(1, pairs):
            pass_copy(i, k).wait_recv()

    for k in range(1, pairs):
        far_copy(0, k).wait_recv()
        pass_copy(0, k).start()
        make_tables(origin(k))
    for k in range(1, pairs):
        pass_copy(0, k).wait_recv()
        make_tables(origin(k, mate))

    def sweep(level, planes, read, base, write, tables):
        low, high = planes
        below = read(low - 1)
        here = read(low)
        for z in range(low, high):
            above = read(z + 1)
            weight = lambda c: tables[level, c, z]
            x = weight(2) * pltpu.roll(here, 7, 0) + weight(3) * pltpu.roll(here, 1, 0)
            y = weight(4) * pltpu.roll(here, 127, 1) + weight(5) * pltpu.roll(here, 1, 1)
            value = base(z, here)
            if above is not None:
                value = value + weight(0) * above
            if below is not None:
                value = value + weight(1) * below
            write(z, value + (x + y))
            below, here = here, above

    def phi(level, load, store, tables=None, scale=None, buffers=None, reach=None, last=None):
        if reach is None:
            full = (0, depth)
            tables, scale, buffers = tab.at[:, :, pl.ds(pad, depth)], scaled, (ping, pong)
            span = lambda sweeps: full
            inside = lambda read: (lambda z: read(z) if 0 <= z < depth else None)
        else:
            span = lambda left: (pad - left - reach, pad + slab + left + reach)
            inside = lambda read: read
        one, two = buffers

        def first(z, v):
            value = v * inverse[level]
            scale[z] = value
            return value

        put = lambda ref: (lambda z, v: ref.__setitem__(z, v))
        get = lambda ref: inside(lambda z: ref[z])
        later = lambda z, v: scale[z]
        reads = [inside(load), get(one), get(two), get(one)]
        writes = [put(one), put(two), put(one), store]
        for n in range(SWEEPS):
            if n == SWEEPS - 1 and last is not None:
                last()
            sweep(level, span(SWEEPS - 1 - n), reads[n],
                  first if n == 0 else later, writes[n], tables)

    def given(c, z):
        return slabs[z // slab, c, z % slab]

    def to_chain(i):
        return lambda z, v: chain.__setitem__((i, pad + z), v + given(force + i, z))

    @pl.when(t == 0)
    def _():
        phi(0, lambda z: given(start, z), lambda z, v: chain.__setitem__((0, pad + z), v))

    forward(1)

    @pl.when(t > 0)
    def _():
        settle(1)
        for z in range(depth):
            chain[0, pad + z] = given(force, z)

    @pl.when(t == 0)
    def _():
        settle(1)
        for z in range(depth):
            chain[0, pad + z] = chain[0, pad + z] + given(force, z)

    phi(0, lambda z: chain[0, pad + z], to_chain(1), last=lambda: forward(2))

    def middle_of():
        forward(3)
        settle(2)

    phi(0, lambda z: chain[1, pad + z], to_chain(2), last=middle_of)
    phi(0, lambda z: chain[2, pad + z], to_chain(3), last=lambda: settle(3))

    half = depth // 2
    low = lax.rem(s, 2) * half
    rows, chain_rows = pl.ds(low, half), pl.ds(pad + low, half)

    def hop_copy(k, source=None):
        return pltpu.make_async_remote_copy(
            chain.at[BLOCK - 1, chain_rows], got.at[t if source is None else source, rows],
            hop_send.at[k - 1], hop_recv.at[t if source is None else source],
            device_id={"tm": lax.rem(t + k, times)}, device_id_type=MESH)

    for k in range(times - 1, 0, -1):
        @pl.when(t + k < times)
        def _():
            hop_copy(k).start()

    ratio = (steps[1] * inverse[1]) / (steps[0] * inverse[0])

    def coarse_tables(z, carry):
        for c in range(6):
            tab[1, c, pad + z] = ratio * tab[0, c, pad + z]
        return carry

    lax.fori_loop(0, depth, coarse_tables, 0)

    def swap_copy(j):
        return remote(got.at[j, rows], swap_send.at[j], swap_recv.at[j], space=mate)

    chain_own = pl.ds(pad + s * slab, slab)

    for j in range(times - 2, -1, -1):
        @pl.when(t > j)
        def _():
            hop_copy(1, j).wait_recv()
            swap_copy(j).start()
            swap_copy(j).wait_recv()

            def again(i, carry):
                source = echo.at[j]
                phi(0, lambda z: source[z], lambda z, v: source.__setitem__(z, v))
                if j == 0:
                    @pl.when(t == 1)
                    def _():
                        out_ref[i] = chain[i, chain_own] + echo[0, own]
                return carry

            echo[j] = got[j]
            lax.fori_loop(0, BLOCK, again, 0)

    @pl.when(t == 0)
    def _():
        for i in range(BLOCK):
            out_ref[i] = chain[i, chain_own]

    @pl.when(t > 1)
    def _():
        for z in range(depth):
            err[1, pad + z] = echo[0, z]

        def correct(m, carry):
            phi(1, lambda z: err[1, pad + z],
                lambda z, v: err.__setitem__((1, pad + z), v + echo[m - 1, z]))
            return carry

        lax.fori_loop(2, t, correct, 0)
        for z in range(depth):
            prev[pad + z] = got[t - 1, z] + err[1, pad + z]

        window = pl.ds(s * slab, slab + 2 * pad)
        near = dict(tables=tab.at[:, :, window], scale=scaled, buffers=(ping, pong))
        points = prev.at[window]
        errors = err.at[1, window]
        added = [chain.at[i, window] for i in range(BLOCK)]
        for i in range(BLOCK - 1):
            reach = (BLOCK - 2 - i) * SWEEPS

            def store(z, v):
                value = v + added[i][z]
                if pad <= z < pad + slab:
                    out_ref[i, z - pad] = value
                if reach:
                    points[z] = v

            phi(0, lambda z: points[z], store, reach=reach, **near)
        gained = echo.at[t - 1, own]

        def finish(z, v):
            out_ref[BLOCK - 1, z - pad] = v + gained[z - pad] + added[BLOCK - 1][z]

        phi(1, lambda z: errors[z], finish, reach=0, **near)

    for i in range(len(pieces)):
        near_copy(i).wait_send()
        for k in range(1, pairs):
            far_copy(i, k).wait_send()
            pass_copy(i, k).wait_send()
    for k in range(1, times):
        @pl.when(t + k < times)
        def _():
            hop_copy(k).wait_send()
    for j in range(times - 1):
        @pl.when(t > j)
        def _():
            swap_copy(j).wait_send()


def shallow_local(forcing, start_field, velocity, diffusivity):
    spaces, times = lax.axis_size("space"), lax.axis_size("tm")
    slab = forcing.shape[1]
    plane = forcing.shape[2:]
    depth, pad = spaces * slab, (BLOCK - 1) * SWEEPS
    dma = pltpu.SemaphoreType.DMA
    vmem = lambda *shape: pltpu.VMEM(shape + plane, jnp.float32)
    padded = depth + 2 * pad
    pieces, pairs = 4, max(spaces // 2 - 1, 1)
    hbm = pl.BlockSpec(memory_space=pltpu.HBM)
    return pl.pallas_call(
        functools.partial(kernel, spaces, times),
        out_shape=pltpu.VMEM(forcing.shape, forcing.dtype),
        in_specs=[hbm] * 3 + [pl.BlockSpec(memory_space=pltpu.SMEM)],
        out_specs=pl.BlockSpec(memory_space=pltpu.VMEM),
        scratch_shapes=[
            vmem(spaces, BLOCK + 4, slab), vmem(2, 6, padded), vmem(padded), vmem(padded),
            vmem(padded), vmem(BLOCK, padded), vmem(times, depth), vmem(times, depth),
            vmem(padded), vmem(2, padded),
            dma((3,)), dma((pieces,)), dma((pieces,)),
            dma((pairs, pieces)), dma((pairs, pieces)), dma((pairs, pieces)), dma((pairs, pieces)),
            dma((times,)), dma((times,)), dma((times,)), dma((times,)),
            pltpu.SemaphoreType.REGULAR((max(times, 3),)),
        ],
        compiler_params=pltpu.CompilerParams(
            collective_id=0, has_side_effects=True),
    )(forcing, start_field, velocity, diffusivity)


def solution(mesh):
    placed = (
        P(("grp", "tm"), "space", None, None),
        P(("grp", "space"), None, None),
        P(None, "space", None, None),
        P("grp"),
    )
    one_level = mesh.shape["tm"] == BLOCK and mesh.shape["space"] % 2 == 0
    return jax.shard_map(
        shallow_local if one_level else deep_local,
        mesh=mesh,
        in_specs=placed,
        out_specs=P(("grp", "tm"), "space", None, None),
        check_vma=False,
    )
```
